32 devices in a mesh: chain: 16 (over z, y, x), grp: 2 (over core).
Axes of the slice: x: 2, y: 2, z: 4, core: 2. Of those that a mesh axis runs over, the one named last changes fastest.
Arguments:
- codes: bfloat16 [2, 16384, 6144], P(None, ('chain', 'grp')), may hold values from -6 to 6
- exponents: int32 [2, 512, 6144], P(None, ('chain', 'grp')), may hold values from -2 to 2
- column_map: int32 [32], replicated, may hold values from 0 to 31, each once
- row_order: int32 [32], replicated, may hold values from 0 to 31, each once
Outputs:
- rollout: bfloat16 [2, 6144, 16384], P(None, ('chain', 'grp'))
- block_sums: float32 [2, 6144, 512], P(None, ('chain', 'grp'))
The draws below stay inside these ranges and needn't reach their ends.
All inputs are finite; a program needn't handle non-finite values.
Results may differ from the reference program's by a relative error of at most 0.001.
Values may be sent and summed in bfloat16 or wider, within the bound.
A program may use at most 128 MiB of HBM per device.

```python
import jax
import jax.numpy as jnp

R = 16384
C = 6144
LAYERS = 2
N_CHAIN = 16
N_GRP = 2


def plant(result, key, low, largest):
    shape = result.shape
    place = [jax.random.randint(jax.random.fold_in(key, axis), (), 0, shape[axis]) for axis in range(len(shape))]
    result = result.at[tuple(place)].set(low)
    longest = shape.index(max(shape))
    place[longest] = (place[longest] + 1) % shape[longest]
    return result.at[tuple(place)].set(largest)


def block_levels(stream_key, extent, pieces, least, largest):
    def one(dim, parts):
        heights = jax.random.uniform(jax.random.fold_in(jax.random.fold_in(stream_key, 6), dim), (parts,), jnp.float32, least / len(pieces), largest / len(pieces))
        return jnp.repeat(jnp.exp(heights), extent[dim] // parts).reshape((-1,) + (1,) * (len(extent) - dim - 1))

    factor_of = one(*pieces[0])
    for cut in pieces[1:]:
        factor_of = factor_of * one(*cut)
    return factor_of


def gaussian(rng, shape, deviation, limit, shards=(), kind=jnp.bfloat16):
    result = jax.random.normal(rng, shape, jnp.float32) * deviation
    if len(shards) > 0:
        result = block_levels(rng, shape, shards, -0.22, 0.18) * result
    return jnp.clip(result, min=-limit, max=limit).astype(kind)


def setup_inputs(seed: int = 0) -> dict:
    arg_keys = jax.random.split(jax.random.key(seed), 5)
    return {
        "codes": gaussian(arg_keys[0], (LAYERS, R, C), 1.0, 6.0, ((1, 32),)),
        "exponents": plant(jax.random.randint(arg_keys[1], (LAYERS, R // 32, C), -2, 3), jax.random.fold_in(arg_keys[1], 1), -2, 2).astype(jnp.int32),
        "column_map": jax.random.permutation(arg_keys[2], N_CHAIN * N_GRP).astype(jnp.int32),
        "row_order": jax.random.permutation(arg_keys[3], N_CHAIN * N_GRP).astype(jnp.int32),
    }


def reference(codes, exponents, column_map, row_order):
    devices = N_CHAIN * N_GRP
    col_width = C // devices
    row_count = R // devices
    scaling = jnp.exp2(exponents.astype(jnp.float32))
    values = (codes.astype(jnp.float32) * jnp.repeat(scaling, 32, axis=1)).astype(jnp.bfloat16)
    col_index = (column_map[:, None] * col_width + jnp.arange(col_width, dtype=jnp.int32)[None, :]).reshape(-1)
    row_index = (row_order[:, None] * row_count + jnp.arange(row_count, dtype=jnp.int32)[None, :]).reshape(-1)
    picked = jnp.take(values, row_index.astype(jnp.int32), axis=1)
    picked = jnp.take(picked, col_index.astype(jnp.int32), axis=2)
    rollout = jnp.transpose(picked, (0, 2, 1))
    block_sums = rollout.astype(jnp.float32).reshape(LAYERS, C, R // 32, 32).sum(axis=-1)
    return rollout, block_sums
```

```python
import functools

import jax
import jax.numpy as jnp
from jax import lax
from jax.experimental import pallas as pl
from jax.experimental.pallas import tpu as pltpu
from jax.sharding import PartitionSpec as P

MESH = pl.DeviceIdType.MESH
BLOCK = 32
LANES = 128


def prepare_kernel(where, codes, exponents, out, held):
    layers, rows, pair = codes.shape
    col_width = pair // 2

    @pl.when(pl.program_id(1) == 0)
    def _():
        for layer in range(layers):
            scaling = jnp.exp2(exponents[layer].astype(jnp.float32)).astype(jnp.bfloat16)
            for first in range(0, rows, LANES):
                pieces = []
                for row in range(first, first + LANES, BLOCK):
                    block = row // BLOCK
                    pieces.append(codes[layer, row : row + BLOCK, :] * scaling[block : block + 1, :])
                turned = jnp.concatenate(pieces, axis=0).T
                out[0, layer, :, first : first + LANES] = turned[:col_width]
                held[layer, :, first : first + LANES] = turned[col_width:]

    @pl.when(pl.program_id(1) == 1)
    def _():
        out[0] = held[...]


def prepare(codes, exponents, column_map, devices):
    layers, rows, width = codes.shape
    col_width = width // devices
    places = jnp.arange(devices, dtype=jnp.int32)
    if col_width % 64 or rows % LANES or devices % 2:
        scaling = jnp.exp2(exponents.astype(jnp.float32))
        values = (codes.astype(jnp.float32) * jnp.repeat(scaling, BLOCK, axis=1)).astype(jnp.bfloat16)
        values = values.reshape(layers, rows, devices, col_width)
        return jnp.take(values.transpose(2, 0, 3, 1), column_map, axis=0)
    where = jnp.sum(jnp.where(column_map[None, :] == places[:, None], places[None, :], 0), axis=1)
    return pl.pallas_call(
        prepare_kernel,
        grid_spec=pltpu.PrefetchScalarGridSpec(
            num_scalar_prefetch=1,
            grid=(devices // 2, 2),
            in_specs=[
                pl.BlockSpec((layers, rows, 2 * col_width), lambda c, j, where: (0, 0, c)),
                pl.BlockSpec((layers, rows // BLOCK, 2 * col_width), lambda c, j, where: (0, 0, c)),
            ],
            out_specs=pl.BlockSpec((1, layers, col_width, rows), lambda c, j, where: (where[2 * c + j], 0, 0, 0)),
            scratch_shapes=[pltpu.VMEM((layers, col_width, rows), jnp.bfloat16)],
        ),
        out_shape=jax.ShapeDtypeStruct((devices, layers, col_width, rows), jnp.bfloat16),
    )(where.astype(jnp.int32), codes, exponents)


def exchange_kernel(devices, grp_size, outgoing, arrived, own, send_sems, recv_sems, own_sems):
    me = lax.axis_index("chain") * grp_size + lax.axis_index("grp")

    def copy_to(step):
        peer = lax.rem(me + step, devices)
        return pltpu.make_async_remote_copy(
            src_ref=outgoing.at[peer],
            dst_ref=arrived.at[me],
            send_sem=send_sems.at[step],
            recv_sem=recv_sems.at[step],
            device_id=(peer // grp_size, lax.rem(peer, grp_size)),
            device_id_type=MESH,
        )

    @pl.loop(1, devices)
    def _(step):
        copy_to(step).start()

    take = pltpu.make_async_copy(outgoing.at[me], own, own_sems.at[0])
    take.start()
    take.wait()
    put = pltpu.make_async_copy(own, arrived.at[me], own_sems.at[1])
    put.start()
    put.wait()

    @pl.loop(1, devices)
    def _(step):
        sender = lax.rem(me - step + devices, devices)
        pltpu.make_async_remote_copy(
            src_ref=outgoing.at[sender],
            dst_ref=arrived.at[sender],
            send_sem=send_sems.at[step],
            recv_sem=recv_sems.at[step],
            device_id=(sender // grp_size, lax.rem(sender, grp_size)),
            device_id_type=MESH,
        ).wait_recv()

    @pl.loop(1, devices)
    def _(step):
        copy_to(step).wait_send()


def exchange(outgoing, devices, grp_size):
    block = outgoing.shape[1:]
    return pl.pallas_call(
        functools.partial(exchange_kernel, devices, grp_size),
        out_shape=jax.ShapeDtypeStruct(outgoing.shape, outgoing.dtype),
        in_specs=[pl.BlockSpec(memory_space=pl.ANY)],
        out_specs=pl.BlockSpec(memory_space=pl.ANY),
        scratch_shapes=[
            pltpu.VMEM(block, outgoing.dtype),
            pltpu.SemaphoreType.DMA((devices,)),
            pltpu.SemaphoreType.DMA((devices,)),
            pltpu.SemaphoreType.DMA((2,)),
        ],
        compiler_params=pltpu.CompilerParams(has_side_effects=True),
    )(outgoing)


def finish_kernel(count, order, *refs):
    arrived, (rollout, sums) = refs[:count], refs[count:]
    rows = arrived[0].shape[-1]
    blocks = rows // BLOCK
    row_block = lax.broadcasted_iota(jnp.int32, (rows, blocks * count), 0) // BLOCK
    column = lax.broadcasted_iota(jnp.int32, (rows, blocks * count), 1)
    total = None
    for part in range(count):
        values = arrived[part][0, 0]
        rollout[0, :, part * rows : (part + 1) * rows] = values
        chooser = jnp.where(column == row_block + part * blocks, 1.0, 0.0).astype(jnp.bfloat16)
        term = jnp.dot(values, chooser, preferred_element_type=jnp.float32)
        total = term if total is None else total + term
    sums[0] = total


def finish(arrived, row_order):
    devices, layers, col_width, rows = arrived.shape
    blocks = rows // BLOCK
    count = max(1, LANES // blocks)
    if rows % LANES or blocks * count != LANES or devices % count or col_width % 16:
        rollout = jnp.take(arrived, row_order, axis=0).transpose(1, 2, 0, 3)
        rollout = rollout.reshape(layers, col_width, devices * rows)
        sums = rollout.astype(jnp.float32).reshape(layers, col_width, devices * blocks, BLOCK).sum(axis=-1)
        return rollout, sums

    def pick(part):
        return lambda layer, group, order: (order[group * count + part], layer, 0, 0)

    return pl.pallas_call(
        functools.partial(finish_kernel, count),
        grid_spec=pltpu.PrefetchScalarGridSpec(
            num_scalar_prefetch=1,
            grid=(layers, devices // count),
            in_specs=[pl.BlockSpec((1, 1, col_width, rows), pick(part)) for part in range(count)],
            out_specs=[
                pl.BlockSpec((1, col_width, count * rows), lambda layer, group, order: (layer, 0, group)),
                pl.BlockSpec((1, col_width, LANES), lambda layer, group, order: (layer, 0, group)),
            ],
        ),
        out_shape=[
            jax.ShapeDtypeStruct((layers, col_width, devices * rows), jnp.bfloat16),
            jax.ShapeDtypeStruct((layers, col_width, devices * blocks), jnp.float32),
        ],
    )(row_order, *([arrived] * count))


def shards(codes, exponents, column_map, row_order):
    grp_size = lax.axis_size("grp")
    devices = lax.axis_size("chain") * grp_size
    outgoing = prepare(codes, exponents, column_map, devices)
    arrived = exchange(outgoing, devices, grp_size)
    rollout, sums = finish(arrived, row_order)
    return (rollout, sums)


def solution(mesh):
    return jax.shard_map(
        shards,
        mesh=mesh,
        in_specs=(P(None, ("chain", "grp"), None), P(None, ("chain", "grp"), None), P(), P()),
        out_specs=(P(None, ("chain", "grp"), None), P(None, ("chain", "grp"), None)),
        check_vma=False,
    )
```

```python
import functools

import jax
import jax.numpy as jnp
from jax import lax
from jax.experimental import pallas as pl
from jax.experimental.pallas import tpu as pltpu
from jax.sharding import PartitionSpec as P

MESH = pl.DeviceIdType.MESH
BLOCK = 32
LANES = 128


def partner(me, step, devices):
    if devices & (devices - 1):
        return lax.rem(me + step, devices)
    peer, bit = 0, 1
    while bit < devices:
        peer = peer + lax.rem(me // bit + step // bit, 2) * bit
        bit *= 2
    return peer


def origin(me, step, devices):
    if devices & (devices - 1):
        return lax.rem(me - step + devices, devices)
    return partner(me, step, devices)


def turn_of(index, devices):
    if devices % 2:
        return index + 1
    odd = lax.rem(index, 2)
    return (index + odd) // 2 + (1 - odd) * (devices // 2)


class Traffic:
    def __init__(self, devices, grp_size, source, arrived, send_sems, recv_sems):
        self.devices, self.grp_size = devices, grp_size
        self.source, self.arrived = source, arrived
        self.send_sems, self.recv_sems = send_sems, recv_sems
        self.me = lax.axis_index("chain") * grp_size + lax.axis_index("grp")

    def copy(self, step, other, slot):
        return pltpu.make_async_remote_copy(
            src_ref=self.source(step, other),
            dst_ref=self.arrived.at[slot],
            send_sem=self.send_sems.at[step],
            recv_sem=self.recv_sems.at[step],
            device_id=(other // self.grp_size, lax.rem(other, self.grp_size)),
            device_id_type=MESH,
        )

    def send(self, step):
        return self.copy(step, partner(self.me, step, self.devices), self.me)

    def finish(self):
        @pl.loop(1, self.devices)
        def _(step):
            sender = origin(self.me, step, self.devices)
            self.copy(step, sender, sender).wait_recv()

        @pl.loop(1, self.devices)
        def _(step):
            self.send(step).wait_send()


def fused_kernel(
    devices, grp_size, column_map, codes, exponents, arrived,
    codes_in, exponents_in, turned, sending, load_sems, send_sems, recv_sems, own_sem,
):
    pairs, layers, rows, pair = codes_in.shape
    col_width = pair // 2

    def loads(index):
        columns = pl.ds(pl.multiple_of(index * pair, LANES), pair)
        return (
            pltpu.make_async_copy(codes.at[:, :, columns], codes_in.at[index], load_sems.at[0, index]),
            pltpu.make_async_copy(exponents.at[:, :, columns], exponents_in.at[index], load_sems.at[1, index]),
        )

    @pl.loop(0, pairs)
    def _(index):
        for load in loads(index):
            load.start()

    @pl.loop(0, pairs)
    def _(index):
        for load in loads(index):
            load.wait()

    traffic = Traffic(
        devices, grp_size, lambda step, other: sending.at[step], arrived, send_sems, recv_sems
    )

    def fill(step):
        column = column_map[partner(traffic.me, step, devices)]
        which = column // 2
        for layer in range(layers):
            scaling = jnp.exp2(exponents_in[which, layer].astype(jnp.float32)).astype(jnp.bfloat16)
            for first in range(0, rows, LANES):
                pieces = []
                for row in range(first, first + LANES, BLOCK):
                    block = row // BLOCK
                    values = codes_in[which, layer, row : row + BLOCK, :]
                    pieces.append(values * scaling[block : block + 1, :])
                both = jnp.concatenate(pieces, axis=0).T
                turned[0, layer, :, first : first + LANES] = both[:col_width]
                turned[1, layer, :, first : first + LANES] = both[col_width:]
        sending[step] = turned[lax.rem(column, 2)]

    fill(turn_of(0, devices))

    @pl.loop(1, devices - 1)
    def _(index):
        fill(turn_of(index, devices))
        traffic.send(turn_of(index - 1, devices)).start()

    fill(0)
    traffic.send(turn_of(devices - 2, devices)).start()
    own = pltpu.make_async_copy(sending.at[0], arrived.at[traffic.me], own_sem)
    own.start()
    own.wait()
    traffic.finish()


def exchange_kernel(devices, grp_size, outgoing, arrived, own, send_sems, recv_sems, own_sems):
    traffic = Traffic(
        devices, grp_size, lambda step, other: outgoing.at[other], arrived, send_sems, recv_sems
    )

    @pl.loop(0, devices - 1)
    def _(index):
        traffic.send(turn_of(index, devices)).start()

    take = pltpu.make_async_copy(outgoing.at[traffic.me], own, own_sems.at[0])
    take.start()
    take.wait()
    put = pltpu.make_async_copy(own, arrived.at[traffic.me], own_sems.at[1])
    put.start()
    put.wait()
    traffic.finish()


def exchange(codes, exponents, column_map, devices, grp_size):
    layers, rows, width = codes.shape
    col_width = width // devices
    block = (layers, col_width, rows)
    shape = jax.ShapeDtypeStruct((devices, *block), jnp.bfloat16)
    anywhere = pl.BlockSpec(memory_space=pl.ANY)
    peers = pltpu.SemaphoreType.DMA((devices,))
    if col_width % 64 or rows % LANES or devices % 2:
        scaling = jnp.exp2(exponents.astype(jnp.float32))
        values = (codes.astype(jnp.float32) * jnp.repeat(scaling, BLOCK, axis=1)).astype(jnp.bfloat16)
        values = values.reshape(layers, rows, devices, col_width)
        outgoing = jnp.take(values.transpose(2, 0, 3, 1), column_map, axis=0)
        return pl.pallas_call(
            functools.partial(exchange_kernel, devices, grp_size),
            out_shape=shape,
            in_specs=[anywhere],
            out_specs=anywhere,
            scratch_shapes=[pltpu.VMEM(block, jnp.bfloat16), peers, peers, pltpu.SemaphoreType.DMA((2,))],
            compiler_params=pltpu.CompilerParams(has_side_effects=True),
        )(outgoing)
    pairs = devices // 2
    return pl.pallas_call(
        functools.partial(fused_kernel, devices, grp_size),
        out_shape=shape,
        in_specs=[pl.BlockSpec(memory_space=pltpu.SMEM), anywhere, anywhere],
        out_specs=anywhere,
        scratch_shapes=[
            pltpu.VMEM((pairs, layers, rows, 2 * col_width), codes.dtype),
            pltpu.VMEM((pairs, layers, rows // BLOCK, 2 * col_width), exponents.dtype),
            pltpu.VMEM((2, *block), jnp.bfloat16),
            pltpu.VMEM((devices, *block), jnp.bfloat16),
            pltpu.SemaphoreType.DMA((2, pairs)),
            peers,
            peers,
            pltpu.SemaphoreType.DMA,
        ],
        compiler_params=pltpu.CompilerParams(has_side_effects=True),
    )(column_map, codes, exponents)


def finish_kernel(count, order, *refs):
    arrived, (rollout, sums) = refs[:count], refs[count:]
    rows = arrived[0].shape[-1]
    blocks = rows // BLOCK
    row_block = lax.broadcasted_iota(jnp.int32, (rows, blocks * count), 0) // BLOCK
    column = lax.broadcasted_iota(jnp.int32, (rows, blocks * count), 1)
    total = None
    for part in range(count):
        values = arrived[part][0, 0]
        rollout[0, :, part * rows : (part + 1) * rows] = values
        chooser = jnp.where(column == row_block + part * blocks, 1.0, 0.0).astype(jnp.bfloat16)
        term = jnp.dot(values, chooser, preferred_element_type=jnp.float32)
        total = term if total is None else total + term
    sums[0] = total


def finish(arrived, row_order):
    devices, layers, col_width, rows = arrived.shape
    blocks = rows // BLOCK
    count = max(1, LANES // blocks)
    if rows % LANES or blocks * count != LANES or devices % count or col_width % 16:
        rollout = jnp.take(arrived, row_order, axis=0).transpose(1, 2, 0, 3)
        rollout = rollout.reshape(layers, col_width, devices * rows)
        sums = rollout.astype(jnp.float32).reshape(layers, col_width, devices * blocks, BLOCK).sum(axis=-1)
        return rollout, sums

    def pick(part):
        return lambda layer, group, order: (order[group * count + part], layer, 0, 0)

    return pl.pallas_call(
        functools.partial(finish_kernel, count),
        grid_spec=pltpu.PrefetchScalarGridSpec(
            num_scalar_prefetch=1,
            grid=(layers, devices // count),
            in_specs=[pl.BlockSpec((1, 1, col_width, rows), pick(part)) for part in range(count)],
            out_specs=[
                pl.BlockSpec((1, col_width, count * rows), lambda layer, group, order: (layer, 0, group)),
                pl.BlockSpec((1, col_width, LANES), lambda layer, group, order: (layer, 0, group)),
            ],
        ),
        out_shape=[
            jax.ShapeDtypeStruct((layers, col_width, devices * rows), jnp.bfloat16),
            jax.ShapeDtypeStruct((layers, col_width, devices * blocks), jnp.float32),
        ],
    )(row_order, *([arrived] * count))


def shards(codes, exponents, column_map, row_order):
    grp_size = lax.axis_size("grp")
    devices = lax.axis_size("chain") * grp_size
    arrived = exchange(codes, exponents, column_map, devices, grp_size)
    rollout, sums = finish(arrived, row_order)
    return (rollout, sums)


def solution(mesh):
    return jax.shard_map(
        shards,
        mesh=mesh,
        in_specs=(P(None, ("chain", "grp"), None), P(None, ("chain", "grp"), None), P(), P()),
        out_specs=(P(None, ("chain", "grp"), None), P(None, ("chain", "grp"), None)),
        check_vma=False,
    )
```

```python
import functools

import jax
import jax.numpy as jnp
from jax import lax
from jax.experimental import pallas as pl
from jax.experimental.pallas import tpu as pltpu
from jax.sharding import PartitionSpec as P

MESH = pl.DeviceIdType.MESH
BLOCK = 32
LANES = 128


def partner(me, step, devices):
    if devices & (devices - 1):
        return lax.rem(me + step, devices)
    peer, bit = 0, 1
    while bit < devices:
        peer = peer + lax.rem(me // bit + step // bit, 2) * bit
        bit *= 2
    return peer


def origin(me, step, devices):
    if devices & (devices - 1):
        return lax.rem(me - step + devices, devices)
    return partner(me, step, devices)


def turn_of(index, devices):
    if devices % 2:
        return index + 1
    odd = lax.rem(index, 2)
    return (index + odd) // 2 + (1 - odd) * (devices // 2)


class Traffic:
    def __init__(self, devices, grp_size, layers, source, arrived, send_sems, recv_sems):
        self.devices, self.grp_size, self.layers = devices, grp_size, layers
        self.source, self.arrived = source, arrived
        self.send_sems, self.recv_sems = send_sems, recv_sems
        self.me = lax.axis_index("chain") * grp_size + lax.axis_index("grp")

    def copy(self, step, layer, other, slot):
        return pltpu.make_async_remote_copy(
            src_ref=self.source(step, layer, other),
            dst_ref=self.arrived.at[slot, layer],
            send_sem=self.send_sems.at[step, layer],
            recv_sem=self.recv_sems.at[step, layer],
            device_id=(other // self.grp_size, lax.rem(other, self.grp_size)),
            device_id_type=MESH,
        )

    def send(self, step, layer):
        return self.copy(step, layer, partner(self.me, step, self.devices), self.me)

    def finish(self):
        @pl.loop(1, self.devices)
        def _(step):
            sender = origin(self.me, step, self.devices)
            for layer in range(self.layers):
                self.copy(step, layer, sender, sender).wait_recv()

        @pl.loop(1, self.devices)
        def _(step):
            for layer in range(self.layers):
                self.send(step, layer).wait_send()


def fused_kernel(devices, grp_size, layers, column_map, codes, exponents, arrived, *scratch):
    codes_in, exponents_in = scratch[:layers], scratch[layers : 2 * layers]
    turned, sending, load_sems, send_sems, recv_sems, own_sem = scratch[2 * layers :]
    pairs, rows, pair = codes_in[0].shape
    col_width = pair // 2

    def loads(layer, index):
        columns = pl.ds(pl.multiple_of(index * pair, LANES), pair)
        return (
            pltpu.make_async_copy(
                codes.at[layer, :, columns], codes_in[layer].at[index], load_sems.at[0, layer, index]
            ),
            pltpu.make_async_copy(
                exponents.at[layer, :, columns], exponents_in[layer].at[index], load_sems.at[1, layer, index]
            ),
        )

    def load(layer):
        @pl.loop(0, pairs)
        def _(index):
            for item in loads(layer, index):
                item.start()

    def loaded(layer):
        @pl.loop(0, pairs)
        def _(index):
            for item in loads(layer, index):
                item.wait()

    traffic = Traffic(
        devices, grp_size, layers, lambda step, layer, other: sending.at[step, layer], arrived, send_sems, recv_sems
    )

    def fill(step, layer):
        column = column_map[partner(traffic.me, step, devices)]
        which = column // 2
        scaling = jnp.exp2(exponents_in[layer][which].astype(jnp.float32)).astype(jnp.bfloat16)
        for first in range(0, rows, LANES):
            pieces = []
            for row in range(first, first + LANES, BLOCK):
                block = row // BLOCK
                pieces.append(codes_in[layer][which, row : row + BLOCK, :] * scaling[block : block + 1, :])
            both = jnp.concatenate(pieces, axis=0).T
            turned[0, :, first : first + LANES] = both[:col_width]
            turned[1, :, first : first + LANES] = both[col_width:]
        sending[step, layer] = turned[lax.rem(column, 2)]

    for layer in range(layers):
        load(layer)
    for layer in range(layers):
        loaded(layer)
        fill(turn_of(0, devices), layer)
        if layer:
            traffic.send(turn_of(0, devices), layer - 1).start()

    @pl.loop(1, devices - 1)
    def _(index):
        for layer in range(layers):
            fill(turn_of(index, devices), layer)
            if layer:
                traffic.send(turn_of(index, devices), layer - 1).start()
            else:
                traffic.send(turn_of(index - 1, devices), layers - 1).start()

    for layer in range(layers):
        fill(0, layer)
    traffic.send(turn_of(devices - 2, devices), layers - 1).start()
    own = pltpu.make_async_copy(sending.at[0], arrived.at[traffic.me], own_sem)
    own.start()
    own.wait()
    traffic.finish()


def exchange_kernel(devices, grp_size, layers, outgoing, arrived, own, send_sems, recv_sems, own_sems):
    traffic = Traffic(
        devices, grp_size, layers, lambda step, layer, other: outgoing.at[other, layer], arrived, send_sems, recv_sems
    )

    @pl.loop(0, devices - 1)
    def _(index):
        for layer in range(layers):
            traffic.send(turn_of(index, devices), layer).start()

    take = pltpu.make_async_copy(outgoing.at[traffic.me], own, own_sems.at[0])
    take.start()
    take.wait()
    put = pltpu.make_async_copy(own, arrived.at[traffic.me], own_sems.at[1])
    put.start()
    put.wait()
    traffic.finish()


def exchange(codes, exponents, column_map, devices, grp_size):
    layers, rows, width = codes.shape
    col_width = width // devices
    block = (layers, col_width, rows)
    shape = jax.ShapeDtypeStruct((devices, *block), jnp.bfloat16)
    anywhere = pl.BlockSpec(memory_space=pl.ANY)
    peers = pltpu.SemaphoreType.DMA((devices, layers))
    if col_width % 64 or rows % LANES or devices % 2:
        scaling = jnp.exp2(exponents.astype(jnp.float32))
        values = (codes.astype(jnp.float32) * jnp.repeat(scaling, BLOCK, axis=1)).astype(jnp.bfloat16)
        values = values.reshape(layers, rows, devices, col_width)
        outgoing = jnp.take(values.transpose(2, 0, 3, 1), column_map, axis=0)
        return pl.pallas_call(
            functools.partial(exchange_kernel, devices, grp_size, layers),
            out_shape=shape,
            in_specs=[anywhere],
            out_specs=anywhere,
            scratch_shapes=[pltpu.VMEM(block, jnp.bfloat16), peers, peers, pltpu.SemaphoreType.DMA((2,))],
            compiler_params=pltpu.CompilerParams(has_side_effects=True),
        )(outgoing)
    pairs = devices // 2
    return pl.pallas_call(
        functools.partial(fused_kernel, devices, grp_size, layers),
        out_shape=shape,
        in_specs=[pl.BlockSpec(memory_space=pltpu.SMEM), anywhere, anywhere],
        out_specs=anywhere,
        scratch_shapes=[
            *[pltpu.VMEM((pairs, rows, 2 * col_width), codes.dtype)] * layers,
            *[pltpu.VMEM((pairs, rows // BLOCK, 2 * col_width), exponents.dtype)] * layers,
            pltpu.VMEM((2, col_width, rows), jnp.bfloat16),
            pltpu.VMEM((devices, *block), jnp.bfloat16),
            pltpu.SemaphoreType.DMA((2, layers, pairs)),
            peers,
            peers,
            pltpu.SemaphoreType.DMA,
        ],
        compiler_params=pltpu.CompilerParams(has_side_effects=True),
    )(column_map, codes, exponents)


def finish_kernel(count, order, *refs):
    arrived, (rollout, sums, chooser) = refs[:count], refs[count:]
    rows = arrived[0].shape[-1]
    blocks = rows // BLOCK

    @pl.when((pl.program_id(0) == 0) & (pl.program_id(1) == 0))
    def _():
        row_block = lax.broadcasted_iota(jnp.int32, (rows, blocks * count), 0) // BLOCK
        column = lax.broadcasted_iota(jnp.int32, (rows, blocks * count), 1)
        for part in range(count):
            chosen = column == row_block + part * blocks
            chooser[part] = jnp.where(chosen, 1.0, 0.0).astype(jnp.bfloat16)

    total = None
    for part in range(count):
        values = arrived[part][0, 0]
        rollout[0, :, part * rows : (part + 1) * rows] = values
        term = jnp.dot(values, chooser[part], preferred_element_type=jnp.float32)
        total = term if total is None else total + term
    sums[0] = total


def finish(arrived, row_order):
    devices, layers, col_width, rows = arrived.shape
    blocks = rows // BLOCK
    count = max(1, LANES // blocks)
    if rows % LANES or blocks * count != LANES or devices % count or col_width % 16:
        rollout = jnp.take(arrived, row_order, axis=0).transpose(1, 2, 0, 3)
        rollout = rollout.reshape(layers, col_width, devices * rows)
        sums = rollout.astype(jnp.float32).reshape(layers, col_width, devices * blocks, BLOCK).sum(axis=-1)
        return rollout, sums

    def pick(part):
        return lambda layer, group, order: (order[group * count + part], layer, 0, 0)

    return pl.pallas_call(
        functools.partial(finish_kernel, count),
        grid_spec=pltpu.PrefetchScalarGridSpec(
            num_scalar_prefetch=1,
            grid=(layers, devices // count),
            in_specs=[pl.BlockSpec((1, 1, col_width, rows), pick(part)) for part in range(count)],
            out_specs=[
                pl.BlockSpec((1, col_width, count * rows), lambda layer, group, order: (layer, 0, group)),
                pl.BlockSpec((1, col_width, LANES), lambda layer, group, order: (layer, 0, group)),
            ],
            scratch_shapes=[pltpu.VMEM((count, rows, LANES), jnp.bfloat16)],
        ),
        out_shape=[
            jax.ShapeDtypeStruct((layers, col_width, devices * rows), jnp.bfloat16),
            jax.ShapeDtypeStruct((layers, col_width, devices * blocks), jnp.float32),
        ],
    )(row_order, *([arrived] * count))


def shards(codes, exponents, column_map, row_order):
    grp_size = lax.axis_size("grp")
    devices = lax.axis_size("chain") * grp_size
    arrived = exchange(codes, exponents, column_map, devices, grp_size)
    rollout, sums = finish(arrived, row_order)
    return (rollout, sums)


def solution(mesh):
    return jax.shard_map(
        shards,
        mesh=mesh,
        in_specs=(P(None, ("chain", "grp"), None), P(None, ("chain", "grp"), None), P(), P()),
        out_specs=(P(None, ("chain", "grp"), None), P(None, ("chain", "grp"), None)),
        check_vma=False,
    )
```
